32 devices in a mesh: dp: 4 (over x, y), tp: 8 (over z, core).
Axes of the slice: x: 2, y: 2, z: 4, core: 2. Of those that a mesh axis runs over, the one named last changes fastest.
Arguments:
- x: bfloat16 [12288, 3584], P(('dp', 'tp')), parts along dimension 0
- dy: bfloat16 [12288, 3584], P(('dp', 'tp')), parts along dimension 0
- gain: bfloat16 [3584], replicated
- wq: bfloat16 [3584, 4096], P(None, 'tp')
- wk: bfloat16 [3584, 2048], P(None, 'tp')
- wv: bfloat16 [3584, 2048], P(None, 'tp')
- wo: bfloat16 [4096, 3584], P('tp')
Outputs:
- output 1: bfloat16 [12288, 3584], P(('dp', 'tp')), parts along dimension 0
- output 2: float32 [4, 3584], P('dp'), parts along dimension 0
- output 3: bfloat16 [14336, 4096], P('dp', 'tp'), parts along dimension 0
- output 4: bfloat16 [14336, 2048], P('dp', 'tp'), parts along dimension 0
- output 5: bfloat16 [14336, 2048], P('dp', 'tp'), parts along dimension 0
- output 6: bfloat16 [16384, 3584], P(('dp', 'tp')), parts along dimension 0
There are 4 independent parts. The reference program is written for one: setup_inputs(seed, part) draws one part's arguments, and reference() takes and returns one part's arrays. A program takes and returns all parts, laid end to end along the dimension named above; an argument that names none is the same for every part.
All inputs are finite; a program needn't handle non-finite values.
Results may differ from the reference program's by a relative error of at most 0.018.
Values are sent between devices in bfloat16 or wider.
A program may use at most 2 GiB of HBM per device.

```python
import jax
import jax.numpy as jnp
from jax import lax

ROWS = 3072
D = 3584
HEADS = 16
KV_HEADS = 8
HEAD = 256
THETA = 10000


def setup_inputs(seed: int = 0, part: int = 0) -> dict:
    kx, ky, kn, kq, kk, kv, ko = jax.random.split(jax.random.key(seed), 7)

    def weights(key, rows, columns):
        return jax.random.normal(key, (rows, columns), jnp.float32) * rows**-0.5

    drawn = {
        "x": jax.random.normal(jax.random.fold_in(kx, part), (ROWS, D), jnp.float32),
        "dy": jax.random.normal(jax.random.fold_in(ky, part), (ROWS, D), jnp.float32) * ROWS**-0.5,
        "gain": 1 + 0.1 * jax.random.normal(kn, (D,), jnp.float32),
        "wq": 2 * weights(kq, D, HEADS * HEAD),
        "wk": 2 * weights(kk, D, KV_HEADS * HEAD),
        "wv": 4 * weights(kv, D, KV_HEADS * HEAD),
        "wo": weights(ko, HEADS * HEAD, D),
    }
    return {k: v.astype(jnp.bfloat16) for k, v in drawn.items()}


def normed(x, gain):
    wide = x.astype(jnp.float32)
    scale = lax.rsqrt(jnp.mean(wide * wide, -1, keepdims=True) + 1e-6)
    return (wide * scale * gain.astype(jnp.float32)).astype(jnp.bfloat16)


def turned(t, place, theta):
    half = t.shape[-1] // 2
    angle = place.astype(jnp.float32)[:, None] * theta ** (-jnp.arange(half, dtype=jnp.float32) / half)
    cos, sin = jnp.cos(angle)[:, None], jnp.sin(angle)[:, None]
    a, b = t[..., :half].astype(jnp.float32), t[..., half:].astype(jnp.float32)
    return jnp.concatenate([a * cos - b * sin, b * cos + a * sin], -1).astype(jnp.bfloat16)


def matmul(a, w):
    return jnp.dot(a, w, preferred_element_type=jnp.float32).astype(jnp.bfloat16)


def einsum(form, a, b):
    return jnp.einsum(form, a.astype(jnp.float32), b.astype(jnp.float32))


def attention(q, k, v):
    scores = einsum("tgsd,ugd->gstu", q, k) * q.shape[-1] ** -0.5
    token = jnp.arange(q.shape[0])
    scores = jnp.where(token[:, None] >= token, scores, -jnp.inf)
    weights = jax.nn.softmax(scores, -1).astype(jnp.bfloat16)
    return einsum("gstu,ugd->tgsd", weights, v).astype(jnp.bfloat16)


def forward(x, gain, wq, wk, wv, wo):
    rows = x.shape[0]
    a, place = normed(x, gain), jnp.arange(rows)
    k = turned(matmul(a, wk).reshape(rows, -1, HEAD), place, THETA)
    q = turned(matmul(a, wq).reshape(rows, -1, HEAD), place, THETA).reshape(rows, k.shape[1], -1, HEAD)
    v = matmul(a, wv).reshape(rows, -1, HEAD)
    seen = attention(q, k, v).reshape(rows, -1)
    return (x.astype(jnp.float32) + jnp.dot(seen, wo, preferred_element_type=jnp.float32)).astype(jnp.bfloat16)


def reference(x, dy, gain, wq, wk, wv, wo):
    _, back = jax.vjp(forward, x, gain.astype(jnp.float32), wq, wk, wv, wo)
    by_x, by_gain, *by_weights = back(dy)
    return (by_x, by_gain[None], *by_weights)
```

```python
import functools

import jax
import jax.numpy as jnp
from jax import lax
from jax.experimental import pallas as pl
from jax.experimental.pallas import tpu as pltpu
from jax.sharding import PartitionSpec as P

NEG = -1e30
HIDDEN = 2 * NEG
LOG2E = 1.4426950408889634
HEAD = 256
THETA = 10000
MESH = pl.DeviceIdType.MESH
NA = 2
NR = 3
TILE = 256
UP, DOWN, PARTNER = 0, 1, 2


def _dot(a, b, ca, cb):
    return lax.dot_general(a, b, (((ca,), (cb,)), ((), ())), preferred_element_type=jnp.float32)


def _kernel(a_own, dy_own, wq, wk, wv, wo, cos, sin,
            full, part, ptin, upin, dnin, sbuf, da_out, dwq, dwk, dwv, dwo,
            w_s, wo_s, cos_s, sin_s, qkv_s, ot_s, lse_s, dk_s, dv_s, g_s, blk_s, da_s, ev_s, at_s, yt_s, wt_s, ut_s,
            mix_s, top_s, dq_s, do_s, dl_s,
            ag_send, ag_line, ag_pt, rs_send, rs_up, rs_dn, pt_send, pt_recv, ld_sem, ev_sem, tl_sem, wt_sem):
    me = lax.axis_index("tp")
    z, c = me // 2, me % 2
    partner = 2 * z + 1 - c
    rows, width = a_own.shape
    piece, slab = rows // NA, rows // NR
    e = HEAD**-0.5 * LOG2E
    scale = HEAD**-0.5

    barrier = pltpu.get_barrier_semaphore()
    for k in range(1, 8):
        pl.semaphore_signal(barrier, inc=1, device_id={"tp": (me + k) % 8}, device_id_type=MESH)
    pl.semaphore_wait(barrier, 7)

    def block(b):
        return pl.ds(pl.multiple_of(b * rows, rows), rows)

    def gather(arr, zb, s, way, src=None):
        at = full.at[arr, pl.ds(pl.multiple_of((2 * zb + c) * rows + s * piece, piece), piece)]
        to = (me + 2, me - 2, partner)[way]
        return pltpu.make_async_remote_copy(
            src_ref=at if src is None else src.at[pl.ds(s * piece, piece)], dst_ref=at,
            send_sem=ag_send.at[way, arr, zb, s], recv_sem=(ag_pt if way == PARTNER else ag_line).at[arr, zb, s],
            device_id={"tp": to}, device_id_type=MESH)

    def wait_partner(arr, zb):
        for s in range(NA):
            gather(arr, zb, s, PARTNER).wait_recv()

    def local(src, dst, sem):
        copy = pltpu.make_async_copy(src, dst, sem)
        copy.start()
        return copy

    def send_own(arr, src, way):
        for s in range(NA):
            gather(arr, z, s, way, src).start()

    @pl.when(z < 3)
    def _():
        send_own(0, a_own, UP)

    @pl.when(z > 0)
    def _():
        send_own(0, a_own, DOWN)

    send_own(0, a_own, PARTNER)

    @pl.when(z == 0)
    def _():
        send_own(1, dy_own, UP)

    @pl.when(z == 3)
    def _():
        send_own(1, dy_own, DOWN)

    send_own(1, dy_own, PARTNER)

    first = [local(a_own, blk_s, ld_sem.at[0]), local(dy_own, da_s, ld_sem.at[1])]
    heads = w_s.shape[1] - 2 * HEAD
    loads = [local(wq, w_s.at[:, pl.ds(0, heads)], ld_sem.at[2]), local(wk, w_s.at[:, pl.ds(heads, HEAD)], ld_sem.at[3]),
             local(wv, w_s.at[:, pl.ds(heads + HEAD, HEAD)], ld_sem.at[4]), local(wo, wo_s, ld_sem.at[5]),
             local(cos, cos_s, ld_sem.at[6]), local(sin, sin_s, ld_sem.at[7])]
    for copy in first:
        copy.wait()
    first = [local(blk_s, full.at[0, block(me)], ld_sem.at[0]), local(da_s, full.at[1, block(me)], ld_sem.at[1])]
    dk_s[...] = jnp.zeros_like(dk_s)
    dv_s[...] = jnp.zeros_like(dv_s)
    for copy in first + loads:
        copy.wait()

    def progress(n, s):
        m = 3 - z

        @pl.when(n <= 2 * z)
        def _():
            arr = jnp.where(n <= z, 0, 1)
            zb = jnp.where(n <= z, z - n, 2 * z - n)
            gather(arr, zb, s, UP).wait_recv()

            @pl.when(z < 3)
            def _():
                gather(arr, zb, s, UP).start()

            gather(arr, zb, s, PARTNER).start()

        @pl.when(n <= 2 * m)
        def _():
            arr = jnp.where(n <= m, 0, 1)
            zb = jnp.where(n <= m, z + n, 4 + m - n)
            gather(arr, zb, s, DOWN).wait_recv()

            @pl.when(z > 0)
            def _():
                gather(arr, zb, s, DOWN).start()

            gather(arr, zb, s, PARTNER).start()

        if s == NA - 1:
            @pl.when((n == z) & (z < 3))
            def _():
                send_own(1, dy_own, UP)

            @pl.when((n == 2 * m) & (z > 0))
            def _():
                send_own(1, dy_own, DOWN)

    def project(b):
        local(full.at[0, block(b)], blk_s, ld_sem.at[0]).wait()

        def columns(t, _):
            r = _dot(blk_s[...], w_s[:, pl.ds(pl.multiple_of(t * HEAD, HEAD), HEAD)], 1, 0).astype(jnp.bfloat16).astype(jnp.float32)
            plain = t == 3
            cs = jnp.where(plain, 1.0, cos_s[block(b), :])
            sn = jnp.where(plain, 0.0, sin_s[block(b), :])
            u, v = r[:, : HEAD // 2], r[:, HEAD // 2 :]
            qkv_s[t, block(b), : HEAD // 2] = (u * cs - v * sn).astype(jnp.bfloat16)
            qkv_s[t, block(b), HEAD // 2 :] = (v * cs + u * sn).astype(jnp.bfloat16)

        lax.fori_loop(0, 4, columns, None)

    def arrivals(n, _):
        @pl.when(n > 0)
        def _():
            for s in range(NA):
                progress(n, s)

        zb = jnp.where(n == 0, z, jnp.where(n == 1, jnp.where(z == 0, 1, z - 1),
                       jnp.where(n == 2, jnp.where(z == 3, 1, jnp.where(z == 2, 3, 2)), jnp.where(z <= 1, 3, 0))))

        def half(h, _):
            @pl.when(h == 1)
            def _():
                wait_partner(0, zb)

            project(2 * zb + jnp.where(h == 0, c, 1 - c))

        lax.fori_loop(0, 2, half, None)

    lax.fori_loop(0, 4, arrivals, None)

    hidden = lax.broadcasted_iota(jnp.int32, (rows, rows), 1) < lax.broadcasted_iota(jnp.int32, (rows, rows), 0)

    def attend(i, _):
        top_s[...] = jnp.full(top_s.shape, NEG, jnp.float32)
        mix_s[...] = jnp.zeros_like(mix_s)
        qs = [qkv_s[h, block(i), :] for h in range(2)]

        def keys(j, masked):
            k, v = qkv_s[2, block(j), :], qkv_s[3, block(j), :]
            values = jnp.concatenate([v.T, jnp.ones((8, rows), jnp.bfloat16)], axis=0)
            scores = [_dot(k, q, 1, 1) for q in qs]
            if masked:
                scores = [jnp.where(hidden, HIDDEN, s) for s in scores]
            ps, keeps = [], []
            for h, s in enumerate(scores):
                old = top_s[h : h + 1, :]
                top = jnp.maximum(old, s.max(axis=0, keepdims=True))
                top_s[h : h + 1, :] = top
                ps.append(jnp.exp2((s - top) * e).astype(jnp.bfloat16))
                keeps.append(jnp.exp2((old - top) * e))
            for h in range(2):
                mix_s[h] = mix_s[h] * keeps[h] + _dot(values, ps[h], 1, 0)

        lax.fori_loop(0, i, lambda j, _: keys(j, False), None)
        keys(i, True)
        for h in range(2):
            total = mix_s[h, HEAD : HEAD + 1, :]
            ot_s[h * HEAD : (h + 1) * HEAD, block(i)] = (mix_s[h, :HEAD, :] * (1 / total)).astype(jnp.bfloat16)
            lse_s[i, h : h + 1, :] = top_s[h : h + 1, :] * e + jnp.log(total) * LOG2E

        @pl.when(i == 5)
        def _():
            progress(4, 0)

    lax.fori_loop(0, 8, attend, None)

    @pl.when(z <= 1)
    def _():
        progress(4, 1)

    def line(zb, s, way):
        at = (zb, pl.ds(pl.multiple_of(s * slab, slab), slab))
        return pltpu.make_async_remote_copy(
            src_ref=sbuf.at[at], dst_ref=(upin, dnin)[way].at[at], send_sem=rs_send.at[zb, s],
            recv_sem=(rs_up, rs_dn)[way].at[zb, s], device_id={"tp": (me + 2, me - 2)[way]}, device_id_type=MESH)

    def across(zb):
        return pltpu.make_async_remote_copy(src_ref=da_s, dst_ref=ptin.at[zb], send_sem=pt_send.at[zb], recv_sem=pt_recv.at[zb],
                                            device_id={"tp": partner}, device_id_type=MESH)

    def event(zb, s):
        at = (zb, pl.ds(pl.multiple_of(s * slab, slab), slab))
        below, above = (z > 0) & (z <= zb), (z < 3) & (z >= zb)

        @pl.when(s == 0)
        def _():
            across(zb).wait_recv()

        one = local(part.at[at], ev_s.at[0], ev_sem.at[0])
        two = local(ptin.at[at], ev_s.at[1], ev_sem.at[1])
        for n, (there, sem, buf, way) in enumerate(((below, rs_up, upin, UP), (above, rs_dn, dnin, DOWN))):
            @pl.when(there)
            def _():
                line(zb, s, way).wait_recv()
                local(buf.at[at], ev_s.at[2 + n], ev_sem.at[2 + n]).wait()

            @pl.when(jnp.logical_not(there))
            def _():
                ev_s[2 + n] = jnp.zeros(ev_s.shape[1:], ev_s.dtype)

        one.wait()
        two.wait()
        total = ev_s[0].astype(jnp.float32) + ev_s[1].astype(jnp.float32) + ev_s[2].astype(jnp.float32) + ev_s[3].astype(jnp.float32)
        ev_s[0] = total.astype(ev_s.dtype)

        @pl.when(z == zb)
        def _():
            local(ev_s.at[0], da_out.at[pl.ds(pl.multiple_of(s * slab, slab), slab)], ev_sem.at[0]).wait()

        @pl.when(z != zb)
        def _():
            local(ev_s.at[0], sbuf.at[at], ev_sem.at[0]).wait()

        @pl.when(z < zb)
        def _():
            line(zb, s, UP).start()

        @pl.when(z > zb)
        def _():
            line(zb, s, DOWN).start()

    def turned_back(d, b):
        cs, sn = cos_s[block(b), :], sin_s[block(b), :]
        u, v = d[:, : HEAD // 2], d[:, HEAD // 2 :]
        return jnp.concatenate([u * cs + v * sn, v * cs - u * sn], 1).astype(jnp.bfloat16)

    def descend(t, _):
        b = 7 - t
        zb, parity = b // 2, b % 2

        @pl.when((t == 2) & (z >= 2))
        def _():
            progress(4, 1)

        @pl.when((t % 2 == 0) & (t >= 2) & (z == 0))
        def _():
            for s in range(NA):
                progress(4 + t // 2, s)

        @pl.when((t % 2 == 0) & (t >= 4) & (z == 3))
        def _():
            for s in range(NA):
                progress(3 + t // 2, s)

        @pl.when(parity != c)
        def _():
            wait_partner(1, zb)

        local(full.at[1, block(b)], blk_s, ld_sem.at[0]).wait()
        for h in range(2):
            d = _dot(wo_s[h * HEAD : (h + 1) * HEAD, :], blk_s[...], 1, 1).astype(jnp.bfloat16)
            do_s[h] = d
            dl_s[h : h + 1, :] = (d.astype(jnp.float32) * ot_s[h * HEAD : (h + 1) * HEAD, block(b)].astype(jnp.float32)).sum(axis=0, keepdims=True)
        dq_s[...] = jnp.zeros_like(dq_s)
        qs = [qkv_s[h, block(b), :] for h in range(2)]

        def keys(j, masked):
            k, v = qkv_s[2, block(j), :], qkv_s[3, block(j), :]
            scores = [_dot(k, q, 1, 1) for q in qs]
            dps = [_dot(v, do_s[h], 1, 0) for h in range(2)]
            ps, dss = [], []
            for h in range(2):
                p = jnp.exp2(scores[h] * e - lse_s[b, h : h + 1, :])
                if masked:
                    p = jnp.where(hidden, 0.0, p)
                ps.append(p.astype(jnp.bfloat16))
                dss.append((p * (dps[h] - dl_s[h : h + 1, :])).astype(jnp.bfloat16))
            kt = k.T
            dv_s[block(j), :] += _dot(ps[0], do_s[0], 1, 1) + _dot(ps[1], do_s[1], 1, 1)
            dk_s[block(j), :] += _dot(dss[0], qs[0], 1, 0) + _dot(dss[1], qs[1], 1, 0)
            for h in range(2):
                dq_s[h] += _dot(kt, dss[h], 1, 0)

        lax.fori_loop(0, b, lambda j, _: keys(j, False), None)
        keys(b, True)
        for h in range(2):
            g_s[block(b), h * HEAD : (h + 1) * HEAD] = turned_back((dq_s[h] * scale).T, b)
        g_s[block(b), heads : heads + HEAD] = turned_back(dk_s[block(b), :] * scale, b)
        g_s[block(b), heads + HEAD :] = dv_s[block(b), :].astype(jnp.bfloat16)

        @pl.when((t > 0) & (parity == c))
        def _():
            across((b + 1) // 2).wait_send()

        def columns(u, _):
            here = pl.ds(pl.multiple_of(u * 512, 512), 512)
            da_s[:, here] = _dot(g_s[block(b), :], w_s[here, :], 1, 1).astype(jnp.bfloat16)

        lax.fori_loop(0, width // 512, columns, None)

        @pl.when(parity == c)
        def _():
            local(da_s, part.at[zb], ld_sem.at[0]).wait()

        @pl.when(parity != c)
        def _():
            across(zb).start()

        @pl.when((parity == 0) & (((z == 0) & (zb > 0)) | ((z == 3) & (zb < 3))))
        def _():
            lax.fori_loop(0, NR, lambda s, _: event(zb, s), None)

    lax.fori_loop(0, 8, descend, None)

    @pl.when(c == 1)
    def _():
        across(0).wait_send()

    tiles = width // TILE

    def fetch(u, slot):
        here = pl.ds(pl.multiple_of(u * TILE, TILE), TILE)
        return (pltpu.make_async_copy(full.at[0, :, here], at_s.at[slot], tl_sem.at[slot, 0]),
                pltpu.make_async_copy(full.at[1, :, here], yt_s.at[slot], tl_sem.at[slot, 1]))

    def put(u):
        here = pl.ds(pl.multiple_of(u * TILE, TILE), TILE)
        return (pltpu.make_async_copy(wt_s.at[:, pl.ds(0, heads)], dwq.at[here, :], wt_sem.at[0]),
                pltpu.make_async_copy(wt_s.at[:, pl.ds(heads, HEAD)], dwk.at[here, :], wt_sem.at[1]),
                pltpu.make_async_copy(wt_s.at[:, pl.ds(heads + HEAD, HEAD)], dwv.at[here, :], wt_sem.at[2]),
                pltpu.make_async_copy(ut_s, dwo.at[:, here], wt_sem.at[3]))

    for copy in fetch(0, 0):
        copy.start()

    def tail(u, _):
        q, s = u // NR, u % NR
        dest = jnp.where(q == 0, 3, jnp.where(q == 1, 3 - z, jnp.where(q == 2, 0, z)))

        @pl.when((u < 4 * NR) & (((z > 0) & (z < 3)) | (q == 3)))
        def _():
            event(dest, s)

        slot = u % 2
        for copy in fetch(u, slot):
            copy.wait()

        @pl.when(u + 1 < tiles)
        def _():
            for copy in fetch(u + 1, 1 - slot):
                copy.start()

        w = _dot(at_s[slot], g_s[...], 0, 0)
        o = _dot(ot_s[...], yt_s[slot], 1, 0)

        @pl.when(u > 0)
        def _():
            for copy in put(u - 1):
                copy.wait()

        wt_s[...] = w.astype(jnp.bfloat16)
        ut_s[...] = o.astype(jnp.bfloat16)
        for copy in put(u):
            copy.start()

    lax.fori_loop(0, tiles, tail, None)
    for copy in put(tiles - 1):
        copy.wait()

    def finish(zb, _):
        for s in range(NA):
            for arr in range(2):
                @pl.when((z < 3) & (zb <= z))
                def _():
                    gather(arr, zb, s, UP).wait_send()

                @pl.when((z > 0) & (zb >= z))
                def _():
                    gather(arr, zb, s, DOWN).wait_send()

                gather(arr, zb, s, PARTNER).wait_send()

        @pl.when(zb != z)
        def _():
            for s in range(NR):
                line(zb, s, UP).wait_send()

    lax.fori_loop(0, 4, finish, None)


def fused(a, dy, wq, wk, wv, wo, cos, sin):
    rows, width = a.shape
    tokens, bf, f32 = 8 * rows, jnp.bfloat16, jnp.float32
    heads = wq.shape[1]
    wide = heads + 2 * HEAD
    shape = jax.ShapeDtypeStruct
    chips = shape((4, rows, width), bf)
    anywhere = pl.BlockSpec(memory_space=pl.ANY)
    out = pl.pallas_call(
        _kernel,
        in_specs=[anywhere] * 8,
        out_specs=[anywhere] * 11,
        out_shape=[shape((2, tokens, width), bf), chips, chips, chips, chips, chips, shape((rows, width), bf),
                   shape(wq.shape, bf), shape(wk.shape, bf), shape(wv.shape, bf), shape(wo.shape, bf)],
        scratch_shapes=[
            pltpu.VMEM((width, wide), bf), pltpu.VMEM((heads, width), bf),
            pltpu.VMEM((tokens, HEAD // 2), f32), pltpu.VMEM((tokens, HEAD // 2), f32),
            pltpu.VMEM((4, tokens, HEAD), bf), pltpu.VMEM((heads, tokens), bf), pltpu.VMEM((8, 8, rows), f32),
            pltpu.VMEM((tokens, HEAD), f32), pltpu.VMEM((tokens, HEAD), f32), pltpu.VMEM((tokens, wide), bf),
            pltpu.VMEM((rows, width), bf), pltpu.VMEM((rows, width), bf), pltpu.VMEM((4, rows // NR, width), bf),
            pltpu.VMEM((2, tokens, TILE), bf), pltpu.VMEM((2, tokens, TILE), bf),
            pltpu.VMEM((TILE, wide), bf), pltpu.VMEM((heads, TILE), bf),
            pltpu.VMEM((2, HEAD + 8, rows), f32), pltpu.VMEM((8, rows), f32), pltpu.VMEM((2, HEAD, rows), f32),
            pltpu.VMEM((2, HEAD, rows), bf), pltpu.VMEM((8, rows), f32),
            pltpu.SemaphoreType.DMA((3, 2, 4, NA)), pltpu.SemaphoreType.DMA((2, 4, NA)), pltpu.SemaphoreType.DMA((2, 4, NA)),
            pltpu.SemaphoreType.DMA((4, NR)), pltpu.SemaphoreType.DMA((4, NR)), pltpu.SemaphoreType.DMA((4, NR)),
            pltpu.SemaphoreType.DMA((4,)), pltpu.SemaphoreType.DMA((4,)), pltpu.SemaphoreType.DMA((8,)),
            pltpu.SemaphoreType.DMA((4,)), pltpu.SemaphoreType.DMA((2, 2)), pltpu.SemaphoreType.DMA((4,)),
        ],
        compiler_params=pltpu.CompilerParams(collective_id=0, has_side_effects=True, vmem_limit_bytes=67043328),
        cost_estimate=pl.CostEstimate(flops=130 * 10**9, bytes_accessed=200 * 10**6, transcendentals=10**7),
    )(a, dy, wq, wk, wv, wo, cos, sin)
    return out[6:]


def normed(x, gain):
    wide = x.astype(jnp.float32)
    scale = lax.rsqrt(jnp.mean(wide * wide, -1, keepdims=True) + 1e-6)
    return (wide * scale * gain.astype(jnp.float32)).astype(jnp.bfloat16)


def solution(mesh):
    def step(x, dy, gain, wq, wk, wv, wo):
        tokens = 8 * x.shape[0]
        half = HEAD // 2
        angle = jnp.arange(tokens).astype(jnp.float32)[:, None] * THETA ** (-jnp.arange(half, dtype=jnp.float32) / half)
        a, back = jax.vjp(normed, x, gain.astype(jnp.float32))
        da, dwq, dwk, dwv, dwo = fused(a, dy, wq, wk, wv, wo, jnp.cos(angle), jnp.sin(angle))
        by_x, by_gain = back(da)
        by_x = (by_x.astype(jnp.float32) + dy.astype(jnp.float32)).astype(jnp.bfloat16)
        return by_x, lax.psum(by_gain, "tp")[None], dwq, dwk, dwv, dwo

    tokens, columns = P(("dp", "tp"), None), P(None, "tp")
    return jax.shard_map(
        step,
        mesh=mesh,
        in_specs=(tokens, tokens, P(None), columns, columns, columns, P("tp", None)),
        out_specs=(tokens, P("dp", None), P("dp", "tp"), P("dp", "tp"), P("dp", "tp"), P(("dp", "tp"), None)),
        check_vma=False,
    )
```

```python
import jax
import jax.numpy as jnp
import numpy as np
from jax import lax
from jax.experimental import pallas as pl
from jax.experimental.pallas import tpu as pltpu
from jax.sharding import PartitionSpec as P

NEG = -1e30
HIDDEN = 2 * NEG
LOG2E = 1.4426950408889634
HEAD = 256
THETA = 10000
MESH = pl.DeviceIdType.MESH
NA = 2
NR = 6
KEPT = 4
TILE = 256
UP, DOWN, PARTNER = 0, 1, 2
PAIR, OTHERS = range(2), range(1, 8)


def loop(steps, body):
    lax.fori_loop(0, steps, body, None)


def _dot(a, b, ca, cb):
    return lax.dot_general(a, b, (((ca,), (cb,)), ((), ())), preferred_element_type=jnp.float32)


def _kernel(x_own, dy_own, gain, wq, wk, wv, wo, angles,
            full, part, ptin, upin, dnin, sbuf, dx_out, dgain, dwq, dwk, dwv, dwo,
            w_s, wo_s, cos_s, sin_s, ang_s, gain_s, qkv_s, ot_s, lse_s, dk_s, dv_s, g_s, gt_s, blk_s, da_s, ev_s, wt_s, ut_s,
            dq_s, do_s, dl_s, dg_s, dgx_s,
            ag_send, ag_line, ag_pt, rs_send, rs_up, rs_dn, pt_send, pt_recv, ld_sem, ev_sem, tl_sem, wt_sem, dg_send, dg_recv):
    me = lax.axis_index("tp")
    z, c = me // 2, me % 2
    partner = 2 * z + 1 - c
    rows, width = x_own.shape
    piece, slab = rows // NA, rows // NR
    e = HEAD**-0.5 * LOG2E
    scale = HEAD**-0.5

    barrier = pltpu.get_barrier_semaphore()
    for k in OTHERS:
        pl.semaphore_signal(barrier, inc=1, device_id={"tp": (me + k) % 8}, device_id_type=MESH)
    pl.semaphore_wait(barrier, 7)

    def block(b):
        return pl.ds(pl.multiple_of(b * rows, rows), rows)

    def gather(arr, zb, s, way, src=None):
        start = jnp.where(arr == 0, (2 * zb + c) * rows + s * piece, (2 * zb + 1 - s) * rows + c * piece)
        at = full.at[arr, pl.ds(pl.multiple_of(start, piece), piece)]
        return pltpu.make_async_remote_copy(
            src_ref=at if src is None else src, dst_ref=at,
            send_sem=ag_send.at[way, arr, zb, s], recv_sem=(ag_pt if way == PARTNER else ag_line).at[arr, zb, s],
            device_id={"tp": (me + 2, me - 2, partner)[way]}, device_id_type=MESH)

    def swap_dy(s):
        at = pl.ds(s * piece, piece)
        return pltpu.make_async_remote_copy(
            src_ref=dy_own.at[at], dst_ref=full.at[1, pl.ds(pl.multiple_of(me * rows + s * piece, piece), piece)],
            send_sem=ag_send.at[PARTNER, 1, z, s], recv_sem=ag_pt.at[1, z, s], device_id={"tp": partner}, device_id_type=MESH)

    def local(src, dst, sem):
        copy = pltpu.make_async_copy(src, dst, sem)
        copy.start()
        return copy

    def send_dy(way):
        for s in range(NA):
            @pl.when(c == 1 - s)
            def _():
                gather(1, z, s, way, dy_own.at[pl.ds((1 - s) * piece, piece)]).start()

            @pl.when(c == s)
            def _():
                gather(1, z, s, way).start()

    for s in range(NA):
        swap_dy(s).start()

    def normed(x):
        wide = x.astype(jnp.float32)
        return wide * lax.rsqrt(jnp.mean(wide * wide, -1, keepdims=True) + 1e-6)

    heads = w_s.shape[1] - 2 * HEAD
    first = [local(x_own.at[pl.ds(s * piece, piece)], blk_s.at[pl.ds(s * piece, piece)], ev_sem.at[0, s]) for s in range(NA)]
    grab = local(gain, gain_s, ev_sem.at[0, 2])
    loads = [local(wq, w_s.at[:, pl.ds(0, heads)], ld_sem.at[2]), local(wk, w_s.at[:, pl.ds(heads, HEAD)], ld_sem.at[3]),
             local(wv, w_s.at[:, pl.ds(heads + HEAD, HEAD)], ld_sem.at[4]), local(wo, wo_s, ld_sem.at[5]),
             local(angles, ang_s, ld_sem.at[6])]
    grab.wait()
    outs = []
    for s in range(NA):
        first[s].wait()

        def strip(r, _):
            here = pl.ds(pl.multiple_of(s * piece + r * 16, 16), 16)
            da_s[here, :] = (normed(blk_s[here, :]) * gain_s[...].astype(jnp.float32)).astype(jnp.bfloat16)

        loop(piece // 16, strip)
        outs.append(local(da_s.at[pl.ds(s * piece, piece)], full.at[0, pl.ds(pl.multiple_of(me * rows + s * piece, piece), piece)],
                          ev_sem.at[0, s]))
    for s in range(NA):
        outs[s].wait()

        @pl.when(z < 3)
        def _():
            gather(0, z, s, UP).start()

        @pl.when(z > 0)
        def _():
            gather(0, z, s, DOWN).start()

        gather(0, z, s, PARTNER).start()

    dk_s[...] = jnp.zeros_like(dk_s)
    dv_s[...] = jnp.zeros_like(dv_s)
    for copy in loads:
        copy.wait()

    for s in range(NA):
        swap_dy(s).wait_recv()

    @pl.when(z == 0)
    def _():
        send_dy(UP)

    @pl.when(z == 3)
    def _():
        send_dy(DOWN)

    def table(r, _):
        here = pl.ds(pl.multiple_of(r * 64, 64), 64)
        cos_hi, sin_hi = ang_s[0, pl.ds(64 + r, 1), :], ang_s[1, pl.ds(64 + r, 1), :]
        cos_lo, sin_lo = ang_s[0, :64, :], ang_s[1, :64, :]
        cos_s[here, :] = cos_hi * cos_lo - sin_hi * sin_lo
        sin_s[here, :] = sin_hi * cos_lo + cos_hi * sin_lo

    loop(8 * rows // 64, table)

    def progress(n, s):
        m = 3 - z

        @pl.when(n <= 2 * z)
        def _():
            arr = jnp.where(n <= z, 0, 1)
            zb = jnp.where(n <= z, z - n, 2 * z - n)
            gather(arr, zb, s, UP).wait_recv()

            @pl.when(z < 3)
            def _():
                gather(arr, zb, s, UP).start()

            gather(arr, zb, s, PARTNER).start()

        @pl.when(n <= 2 * m)
        def _():
            arr = jnp.where(n <= m, 0, 1)
            zb = jnp.where(n <= m, z + n, 4 + m - n)
            gather(arr, zb, s, DOWN).wait_recv()

            @pl.when(z > 0)
            def _():
                gather(arr, zb, s, DOWN).start()

            gather(arr, zb, s, PARTNER).start()

        if isinstance(s, int) and s == NA - 1:
            @pl.when((n == z) & (z < 3))
            def _():
                send_dy(UP)

            @pl.when((n == 2 * m) & (z > 0))
            def _():
                send_dy(DOWN)

    def project(b):
        local(full.at[0, block(b)], blk_s, ld_sem.at[0]).wait()

        def columns(t, _):
            r = _dot(blk_s[...], w_s[:, pl.ds(pl.multiple_of(t * HEAD, HEAD), HEAD)], 1, 0).astype(jnp.bfloat16).astype(jnp.float32)
            plain = t == 3
            cs = jnp.where(plain, 1.0, cos_s[block(b), :])
            sn = jnp.where(plain, 0.0, sin_s[block(b), :])
            u, v = r[:, : HEAD // 2], r[:, HEAD // 2 :]
            qkv_s[t, block(b), : HEAD // 2] = (u * cs - v * sn).astype(jnp.bfloat16)
            qkv_s[t, block(b), HEAD // 2 :] = (v * cs + u * sn).astype(jnp.bfloat16)

        loop(4, columns)

    hidden = lax.broadcasted_iota(jnp.int32, (rows, rows), 1) < lax.broadcasted_iota(jnp.int32, (rows, rows), 0)

    def turn(zb):
        one = jnp.where(zb == 1, 0, jnp.where(zb == 0, 1, zb))
        two = jnp.where(zb == 2, 0, jnp.where(zb == 1, 1, jnp.where(zb == 3, 2, 3)))
        return jnp.where(z == 0, zb, jnp.where(z == 1, one, jnp.where(z == 2, two, 3 - zb)))

    def forward(mix_s, top_s):
        top_s[...] = jnp.full(top_s.shape, NEG, jnp.float32)
        mix_s[...] = jnp.zeros_like(mix_s)

        def scored(i, j, masked):
            k, v = qkv_s[2, block(j), :], qkv_s[3, block(j), :]
            values = jnp.concatenate([v.T, jnp.ones((8, rows), jnp.bfloat16)], axis=0)
            scores = [_dot(k, qkv_s[h, block(i), :], 1, 1) for h in PAIR]
            if masked:
                scores = [jnp.where(hidden, HIDDEN, s) for s in scores]
            ps, keeps = [], []
            for h, s in enumerate(scores):
                old = top_s[i, h : h + 1, :]
                top = jnp.maximum(old, s.max(axis=0, keepdims=True))
                top_s[i, h : h + 1, :] = top
                ps.append(jnp.exp2((s - top) * e).astype(jnp.bfloat16))
                keeps.append(jnp.exp2((old - top) * e))
            for h in PAIR:
                mix_s[i, h] = mix_s[i, h] * keeps[h] + _dot(values, ps[h], 1, 0)

        def arrivals(n, _):
            @pl.when(n > 0)
            def _():
                for s in range(NA):
                    progress(n, s)

            zb = jnp.where(n == 0, z, jnp.where(n == 1, jnp.where(z == 0, 1, z - 1),
                           jnp.where(n == 2, jnp.where(z == 3, 1, jnp.where(z == 2, 3, 2)), jnp.where(z <= 1, 3, 0))))

            def half(h, _):
                @pl.when(h == 1)
                def _():
                    for s in range(NA):
                        gather(0, zb, s, PARTNER).wait_recv()

                b = 2 * zb + jnp.where(h == 0, c, 1 - c)
                project(b)
                scored(b, b, True)

                def other(j, _):
                    there = 2 * turn(j // 2) + jnp.where(j % 2 == c, 0, 1)

                    @pl.when(there < 2 * n + h)
                    def _():
                        scored(jnp.maximum(b, j), jnp.minimum(b, j), False)

                loop(8, other)

            loop(2, half)

        loop(4, arrivals)

        def close(i, _):
            for h in PAIR:
                total = mix_s[i, h, HEAD : HEAD + 1, :]
                ot_s[h * HEAD : (h + 1) * HEAD, block(i)] = (mix_s[i, h, :HEAD, :] * (1 / total)).astype(jnp.bfloat16)
                lse_s[i, h : h + 1, :] = top_s[i, h : h + 1, :] * e + jnp.log(total) * LOG2E

        loop(8, close)

    pl.run_scoped(forward, pltpu.VMEM((8, 2, HEAD + 8, rows), jnp.float32), pltpu.VMEM((8, 8, rows), jnp.float32))

    def line(zb, s, way):
        at = (zb, pl.ds(pl.multiple_of(s * slab, slab), slab))
        return pltpu.make_async_remote_copy(
            src_ref=sbuf.at[at], dst_ref=(upin, dnin)[way].at[at], send_sem=rs_send.at[zb, s],
            recv_sem=(rs_up, rs_dn)[way].at[zb, s], device_id={"tp": (me + 2, me - 2)[way]}, device_id_type=MESH)

    def across(zb, here=slice(None)):
        return pltpu.make_async_remote_copy(src_ref=da_s.at[:, here], dst_ref=ptin.at[zb, :, here], send_sem=pt_send.at[zb], recv_sem=pt_recv.at[zb],
                                            device_id={"tp": partner}, device_id_type=MESH)

    def keep(s, slot):
        return pltpu.make_async_copy(ev_s.at[slot, 0], dx_out.at[pl.ds(pl.multiple_of(s * slab, slab), slab)], ld_sem.at[7])

    def event(zb, s, lo=0, hi=NR):
        slot = s % 2
        below, above = (z > 0) & (z <= zb), (z < 3) & (z >= zb)

        def place(s):
            return zb, pl.ds(pl.multiple_of(s * slab, slab), slab)

        def terms(s, slot):
            return (pltpu.make_async_copy(part.at[place(s)], ev_s.at[slot, 0], ev_sem.at[slot, 0]),
                    pltpu.make_async_copy(ptin.at[place(s)], ev_s.at[slot, 1], ev_sem.at[slot, 1]))

        @pl.when((z == zb) & (s > 0))
        def _():
            keep(s - 1, 1 - slot).wait()

        @pl.when(jnp.equal(s, 0))
        def _():
            across(zb).wait_recv()

        @pl.when(jnp.equal(s, lo))
        def _():
            for copy in terms(s, slot):
                copy.start()

        @pl.when(s + 1 < hi)
        def _():
            for copy in terms(s + 1, 1 - slot):
                copy.start()

        sides = ((2, below, rs_up, upin, UP), (3, above, rs_dn, dnin, DOWN))
        for n, there, sem, buf, way in sides:
            @pl.when(there)
            def _():
                line(zb, s, way).wait_recv()
                local(buf.at[place(s)], ev_s.at[slot, n], ev_sem.at[slot, n])

            @pl.when(jnp.logical_not(there))
            def _():
                ev_s[slot, n] = jnp.zeros(ev_s.shape[2:], ev_s.dtype)

        for copy in terms(s, slot):
            copy.wait()
        for n, there, sem, buf, way in sides:
            @pl.when(there)
            def _():
                pltpu.make_async_copy(buf.at[place(s)], ev_s.at[slot, n], ev_sem.at[slot, n]).wait()

        def total(here):
            return (ev_s[slot, 0, here, :].astype(jnp.float32) + ev_s[slot, 1, here, :].astype(jnp.float32)
                    + ev_s[slot, 2, here, :].astype(jnp.float32) + ev_s[slot, 3, here, :].astype(jnp.float32))

        @pl.when(z == zb)
        def _():
            def strip(r, _):
                here = pl.ds(pl.multiple_of(r * 16, 16), 16)
                mine = pl.ds(pl.multiple_of(s * slab + r * 16, 16), 16)
                da = total(here)
                wide = blk_s[mine, :].astype(jnp.float32)
                scale = lax.rsqrt(jnp.mean(wide * wide, -1, keepdims=True) + 1e-6)
                unit = wide * scale
                each = da * unit
                dg_s[...] += each[:8, :] + each[8:, :]
                d = da * gain_s[...].astype(jnp.float32)
                dx = (d - unit * jnp.mean(d * unit, -1, keepdims=True)) * scale
                ev_s[slot, 0, here, :] = (dx + da_s[mine, :].astype(jnp.float32)).astype(ev_s.dtype)

            loop(slab // 16, strip)
            keep(s, slot).start()

        @pl.when(z != zb)
        def _():
            def strip(r, _):
                here = pl.ds(pl.multiple_of(r * 16, 16), 16)
                ev_s[slot, 0, here, :] = total(here).astype(ev_s.dtype)

            loop(slab // 16, strip)
            local(ev_s.at[slot, 0], sbuf.at[place(s)], ev_sem.at[slot, 0]).wait()

        @pl.when(z < zb)
        def _():
            line(zb, s, UP).start()

        @pl.when(z > zb)
        def _():
            line(zb, s, DOWN).start()

    def turned_back(d, b):
        cs, sn = cos_s[block(b), :], sin_s[block(b), :]
        u, v = d[:, : HEAD // 2], d[:, HEAD // 2 :]
        return jnp.concatenate([u * cs + v * sn, v * cs - u * sn], 1).astype(jnp.bfloat16)

    def begin(zb):
        @pl.when(((z == 0) & (zb > 0)) | ((z == 3) & (zb < 3)))
        def _():
            stop = jnp.where((z == 3) & (zb > 0), KEPT, NR)
            loop(stop, lambda s, _: event(zb, s, 0, stop))

    def later(zb):
        return (c == 1) | ((z == 0) & (zb == 1))

    def descend(t, _):
        b = 7 - t
        zb, parity = b // 2, b % 2

        @pl.when((t == 2) & (z > 0) & (z < 3))
        def _():
            for s in range(NA):
                progress(4, s)

        coming = (zb != z) & ((z == 0) | (z == 3))

        @pl.when(coming)
        def _():
            progress(jnp.where(z == 0, 4, 3) + t // 2, t % 2)

        def fetch_dy(b):
            @pl.when(zb != z)
            def _():
                gather(1, zb, 1 - b % 2, PARTNER).wait_recv()

            @pl.when(b == me)
            def _():
                local(dy_own, blk_s, ld_sem.at[0])

            @pl.when(b != me)
            def _():
                local(full.at[1, block(b)], blk_s, ld_sem.at[0])

        @pl.when((t % 2 == 0) | coming)
        def _():
            fetch_dy(b)

        pltpu.make_async_copy(full.at[1, block(b)], blk_s, ld_sem.at[0]).wait()

        @pl.when(b == me)
        def _():
            local(blk_s, full.at[1, block(me)], ld_sem.at[1])

        for h in PAIR:
            d = _dot(wo_s[h * HEAD : (h + 1) * HEAD, :], blk_s[...], 1, 1).astype(jnp.bfloat16)
            do_s[h] = d
            dl_s[h : h + 1, :] = (d.astype(jnp.float32) * ot_s[h * HEAD : (h + 1) * HEAD, block(b)].astype(jnp.float32)).sum(axis=0, keepdims=True)
        dq_s[...] = jnp.zeros_like(dq_s)
        qs = [qkv_s[h, block(b), :] for h in PAIR]

        def keys(j, masked):
            k, v = qkv_s[2, block(j), :], qkv_s[3, block(j), :]
            scores = [_dot(k, q, 1, 1) for q in qs]
            dps = [_dot(v, do_s[h], 1, 0) for h in PAIR]
            ps, dss = [], []
            for h in PAIR:
                p = jnp.exp2(scores[h] * e - lse_s[b, h : h + 1, :])
                if masked:
                    p = jnp.where(hidden, 0.0, p)
                ps.append(p.astype(jnp.bfloat16))
                dss.append((p * (dps[h] - dl_s[h : h + 1, :])).astype(jnp.bfloat16))
            kt = k.T
            dv_s[block(j), :] += _dot(ps[0], do_s[0], 1, 1) + _dot(ps[1], do_s[1], 1, 1)
            dk_s[block(j), :] += _dot(dss[0], qs[0], 1, 0) + _dot(dss[1], qs[1], 1, 0)
            for h in PAIR:
                dq_s[h] += _dot(kt, dss[h], 1, 0)

        keys(b, True)

        @pl.when(b == me)
        def _():
            pltpu.make_async_copy(blk_s, full.at[1, block(me)], ld_sem.at[1]).wait()

        @pl.when((t % 2 == 0) & jnp.logical_not(coming))
        def _():
            fetch_dy(b - 1)

        loop(b, lambda j, _: keys(j, False))

        @pl.when((t > 0) & (parity != c) & later((b + 1) // 2))
        def _():
            begin((b + 1) // 2)

        grads = [turned_back((dq_s[h] * scale).T, b) for h in PAIR]
        grads += [turned_back(dk_s[block(b), :] * scale, b), dv_s[block(b), :].astype(jnp.bfloat16)]
        for n, grad in enumerate(grads):
            g_s[:, n * HEAD : (n + 1) * HEAD] = grad
            gt_s[n * HEAD : (n + 1) * HEAD, block(b)] = grad.T

        @pl.when((t > 0) & (parity == c))
        def _():
            across((b + 1) // 2).wait_send()

        def pass_on(u):
            @pl.when((parity != c) & (u >= 0))
            def _():
                across(zb, pl.ds(pl.multiple_of(u * 512, 512), 512)).start()

        def columns(u, _):
            here = pl.ds(pl.multiple_of(u * 512, 512), 512)
            da_s[:, here] = _dot(g_s[...], w_s[here, :], 1, 1).astype(jnp.bfloat16)
            pass_on(u - 1)

        loop(width // 512, columns)
        pass_on(width // 512 - 1)

        @pl.when(parity == c)
        def _():
            local(da_s, part.at[zb], ld_sem.at[1]).wait()

        @pl.when((parity == c) & jnp.logical_not(later(zb)))
        def _():
            begin(zb)

    loop(8, descend)

    @pl.when(z == 3)
    def _():
        for zb in (1, 2):
            lax.fori_loop(KEPT, NR, lambda s, _: event(zb, s, KEPT), None)

    @pl.when(c == 1)
    def _():
        across(0).wait_send()

    tiles = width // TILE
    dg_s[...] = jnp.zeros_like(dg_s)
    mine = [local(x_own, blk_s, ld_sem.at[0]), local(dy_own, da_s, ld_sem.at[1])]

    def weights(at_s, yt_s):
        def fetch(u, slot):
            here = pl.ds(pl.multiple_of(u * TILE, TILE), TILE)
            return (pltpu.make_async_copy(full.at[0, :, here], at_s.at[slot], tl_sem.at[slot, 0]),
                    pltpu.make_async_copy(full.at[1, :, here], yt_s.at[slot], tl_sem.at[slot, 1]))

        def put(u):
            here = pl.ds(pl.multiple_of(u * TILE, TILE), TILE)
            return (pltpu.make_async_copy(wt_s.at[:, pl.ds(0, heads)], dwq.at[here, :], wt_sem.at[0]),
                    pltpu.make_async_copy(wt_s.at[:, pl.ds(heads, HEAD)], dwk.at[here, :], wt_sem.at[1]),
                    pltpu.make_async_copy(wt_s.at[:, pl.ds(heads + HEAD, HEAD)], dwv.at[here, :], wt_sem.at[2]),
                    pltpu.make_async_copy(ut_s, dwo.at[:, here], wt_sem.at[3]))

        for copy in fetch(0, 0):
            copy.start()

        def tail(u, _):
            slot = u % 2
            for copy in fetch(u, slot):
                copy.wait()

            @pl.when(u + 1 < tiles)
            def _():
                for copy in fetch(u + 1, 1 - slot):
                    copy.start()

            w = _dot(gt_s[...], at_s[slot], 1, 0)
            o = _dot(ot_s[...], yt_s[slot], 1, 0)

            @pl.when(u > 0)
            def _():
                for copy in put(u - 1):
                    copy.wait()

            wt_s[...] = w.astype(jnp.bfloat16).T
            ut_s[...] = o.astype(jnp.bfloat16)
            for copy in put(u):
                copy.start()

            @pl.when((z == 1) & (u < 2 * NR))
            def _():
                event(jnp.where(u < NR, 3, 2), u % NR)

            v = u // 2 - 1

            @pl.when((z == 2) & (u % 2 == 1) & (v >= 0))
            def _():
                lax.fori_loop(jnp.where(v < KEPT, 0, 1), 2, lambda k, _: event(1 + 2 * k, v, v, v + 1), None)

        loop(tiles, tail)
        for copy in put(tiles - 1):
            copy.wait()

    pl.run_scoped(weights, pltpu.VMEM((2, 8 * rows, TILE), jnp.bfloat16), pltpu.VMEM((2, 8 * rows, TILE), jnp.bfloat16))
    for copy in mine:
        copy.wait()

    @pl.when((z > 0) & (z < 3))
    def _():
        loop(NR, lambda s, _: event(0, s))

    @pl.when(z == 2)
    def _():
        lax.fori_loop(KEPT, NR, lambda s, _: event(1, s, KEPT), None)

    loop(NR, lambda s, _: event(z, s))
    keep(NR - 1, (NR - 1) % 2).wait()
    dgx_s[me] = dg_s[...].sum(axis=0, keepdims=True)

    def share(k):
        to = (me + k) % 8
        return pltpu.make_async_remote_copy(src_ref=dgx_s.at[me], dst_ref=dgx_s.at[me], send_sem=dg_send.at[k], recv_sem=dg_recv.at[8 - k],
                                            device_id={"tp": to}, device_id_type=MESH)

    for k in OTHERS:
        share(k).start()
    for k in OTHERS:
        pltpu.make_async_remote_copy(src_ref=dgx_s.at[me], dst_ref=dgx_s.at[(me + k) % 8], send_sem=dg_send.at[k], recv_sem=dg_recv.at[k],
                                     device_id={"tp": (me + k) % 8}, device_id_type=MESH).wait_recv()
    whole = dgx_s[0]
    for k in OTHERS:
        whole = whole + dgx_s[k]
    dg_s[0:1, :] = whole
    local(dg_s.at[pl.ds(0, 1)], dgain, ev_sem.at[0, 0]).wait()
    for k in OTHERS:
        share(k).wait_send()

    def finish(zb, _):
        for s in range(NA):
            for arr in PAIR:
                @pl.when((z < 3) & (zb <= z))
                def _():
                    gather(arr, zb, s, UP).wait_send()

                @pl.when((z > 0) & (zb >= z))
                def _():
                    gather(arr, zb, s, DOWN).wait_send()

                gather(arr, zb, s, PARTNER).wait_send()

        @pl.when(zb != z)
        def _():
            for s in range(NR):
                line(zb, s, UP).wait_send()

    loop(4, finish)


def fused(x, dy, gain, wq, wk, wv, wo):
    rows, width = x.shape
    tokens, bf, f32 = 8 * rows, jnp.bfloat16, jnp.float32
    heads = wq.shape[1]
    wide = heads + 2 * HEAD
    place = np.concatenate([np.arange(64), np.arange(0, tokens, 64)]).astype(np.float64)
    angle = place[:, None] * float(THETA) ** (-np.arange(HEAD // 2) / (HEAD // 2))
    angles = jnp.asarray(np.stack([np.cos(angle), np.sin(angle)]).astype(np.float32))
    shape = jax.ShapeDtypeStruct
    chips = shape((4, rows, width), bf)
    anywhere = pl.BlockSpec(memory_space=pl.ANY)
    out = pl.pallas_call(
        _kernel,
        in_specs=[anywhere] * 8,
        out_specs=[anywhere] * 12,
        out_shape=[shape((2, tokens, width), bf), chips, chips, chips, chips, chips, shape((rows, width), bf), shape((1, width), f32),
                   shape(wq.shape, bf), shape(wk.shape, bf), shape(wv.shape, bf), shape(wo.shape, bf)],
        scratch_shapes=[
            pltpu.VMEM((width, wide), bf), pltpu.VMEM((heads, width), bf),
            pltpu.VMEM((tokens, HEAD // 2), f32), pltpu.VMEM((tokens, HEAD // 2), f32), pltpu.VMEM(angles.shape, f32), pltpu.VMEM((1, width), bf),
            pltpu.VMEM((4, tokens, HEAD), bf), pltpu.VMEM((heads, tokens), bf), pltpu.VMEM((8, 8, rows), f32),
            pltpu.VMEM((tokens, HEAD), f32), pltpu.VMEM((tokens, HEAD), f32), pltpu.VMEM((rows, wide), bf), pltpu.VMEM((wide, tokens), bf),
            pltpu.VMEM((rows, width), bf), pltpu.VMEM((rows, width), bf), pltpu.VMEM((2, 4, rows // NR, width), bf),
            pltpu.VMEM((TILE, wide), bf), pltpu.VMEM((heads, TILE), bf),
            pltpu.VMEM((2, HEAD, rows), f32), pltpu.VMEM((2, HEAD, rows), bf), pltpu.VMEM((8, rows), f32),
            pltpu.VMEM((8, width), f32), pltpu.VMEM((8, 1, width), f32),
            pltpu.SemaphoreType.DMA((3, 2, 4, NA)), pltpu.SemaphoreType.DMA((2, 4, NA)), pltpu.SemaphoreType.DMA((2, 4, NA)),
            pltpu.SemaphoreType.DMA((4, NR)), pltpu.SemaphoreType.DMA((4, NR)), pltpu.SemaphoreType.DMA((4, NR)),
            pltpu.SemaphoreType.DMA((4,)), pltpu.SemaphoreType.DMA((4,)), pltpu.SemaphoreType.DMA((8,)),
            pltpu.SemaphoreType.DMA((2, 4)), pltpu.SemaphoreType.DMA((2, 2)), pltpu.SemaphoreType.DMA((4,)),
            pltpu.SemaphoreType.DMA((8,)), pltpu.SemaphoreType.DMA((8,)),
        ],
        compiler_params=pltpu.CompilerParams(collective_id=0, has_side_effects=True, vmem_limit_bytes=67043328),
        cost_estimate=pl.CostEstimate(flops=130 * 10**9, bytes_accessed=200 * 10**6, transcendentals=10**7),
    )(x, dy, gain[None], wq, wk, wv, wo, angles)
    return out[6:]


def solution(mesh):
    tokens, columns = P(("dp", "tp"), None), P(None, "tp")
    return jax.shard_map(
        fused,
        mesh=mesh,
        in_specs=(tokens, tokens, P(None), columns, columns, columns, P("tp", None)),
        out_specs=(tokens, P("dp", None), P("dp", "tp"), P("dp", "tp"), P("dp", "tp"), P(("dp", "tp"), None)),
        check_vma=False,
    )
```
